32 devices in a mesh: blk: 8 (over z, x), rep: 4 (over y, core).
Axes of the slice: x: 2, y: 2, z: 4, core: 2. Of those that a mesh axis runs over, the one named last changes fastest.
Arguments:
- query_embed: bfloat16 [8, 4, 256, 256], P('blk', 'rep'), may hold values from -96 to 96
- positive_ids: int32 [8, 4, 256], P('blk'), may hold values from 0 to 2047, as said below
- pair_blocks: int32 [8, 8], P('blk'), may hold values from 0 to 31, as said below
- code_ids: int32 [8, 4, 8, 64], P('blk', 'rep'), may hold values from 0 to 255
- codebooks: bfloat16 [2048, 256], replicated, may hold values from -3 to 3
Outputs:
- query_loss: float32 [8, 4, 256], P('blk', 'rep')
- query_grad: float32 [8, 4, 256, 256], P('blk', 'rep')
- passage_grad: float32 [8, 4, 64, 256], P('blk', 'rep')
- codebook_grad: float32 [2048, 256], P(('blk', 'rep'))
The draws below stay inside these ranges and needn't reach their ends.
Inputs may be any that keep to these rules, and one draw needn't show every extreme that they name: `pair_blocks`: each row names 8 different passage blocks; at most 2 of them belong to one owner o (blocks o * 4 to o * 4 + 3), and in every row some owner has exactly 2. Some blocks are named in many rows. `positive_ids`: the positive passage of a query lies in a block named in its query block's row of pair_blocks.
All inputs are finite; a program needn't handle non-finite values.
Results may differ from the reference program's by a relative error of at most 0.0079.
Values may be sent and summed in bfloat16 or wider, within the bound.
A program may use at most 64 MiB of HBM per device.

```python
import jax
import jax.numpy as jnp
from jax import lax

E = 256
BOOKS = 8
CODES = 256
QR = 256
PR = 16
PBLK_DEV = 4
CAP = 2
N_BLK = 8
N_REP = 4


def pair_table(key):
    base = jax.random.fold_in(key, 7001)
    first, second, third = jax.random.split(base, 3)
    partition_overall_sum = PBLK_DEV * N_BLK
    extreme_value_perturbation = jax.random.randint(first, (N_BLK, partition_overall_sum), 0, 1 << 20)
    discretization_tier = jax.random.randint(second, (partition_overall_sum,), 0, 4) * (1 << 18)
    shift = jax.random.randint(third, (), 0, N_BLK)
    holding_accelerator = jnp.arange(partition_overall_sum, dtype=jnp.int32) // PBLK_DEV
    imposed_selection = (jnp.arange(N_BLK, dtype=jnp.int32) * 5 + shift) % N_BLK
    hinge_offset = (holding_accelerator[None, :] == imposed_selection[:, None]).astype(jnp.int32) * (1 << 30)
    similarity_logit = (extreme_value_perturbation + discretization_tier[None, :]) * partition_overall_sum + jnp.arange(partition_overall_sum, dtype=jnp.int32)[None, :] + hinge_offset
    grouped = similarity_logit.reshape(N_BLK, N_BLK, PBLK_DEV)
    best, where_at = lax.top_k(grouped, CAP)
    block_ids = jnp.arange(N_BLK, dtype=jnp.int32)[None, :, None] * PBLK_DEV + where_at
    flat_best = best.reshape(N_BLK, N_BLK * CAP)
    flat_ids = block_ids.reshape(N_BLK, N_BLK * CAP)
    unused, picked = lax.top_k(flat_best, N_BLK)
    return jnp.take_along_axis(flat_ids, picked, axis=1).astype(jnp.int32)


def positive_table(key, pairs_drawn):
    base = jax.random.fold_in(key, 7002)
    first, second = jax.random.split(base)
    slot_pick = jax.random.randint(first, (N_BLK, N_REP * QR), 0, N_BLK)
    row_pick = jax.random.randint(second, (N_BLK, N_REP * QR), 0, PR * N_REP)
    chosen = jnp.take_along_axis(pairs_drawn, slot_pick, axis=1)
    return (chosen * (PR * N_REP) + row_pick).reshape(N_BLK, N_REP, QR).astype(jnp.int32)


def code_table(key):
    return jax.random.randint(jax.random.fold_in(key, 7003), (N_BLK, N_REP, BOOKS, PBLK_DEV * PR), 0, CODES).astype(jnp.int32)


def book_table(key):
    values = jax.random.normal(jax.random.fold_in(key, 7004), (BOOKS * CODES, E), jnp.float32) * 0.5
    return jnp.clip(values, -3.0, 3.0).astype(jnp.bfloat16)


def draw_pair_blocks(key, part):
    return pair_table(key)


def draw_positive_ids(key, part):
    return positive_table(key, pair_table(key))


def draw_code_ids(key, part):
    return code_table(key)


def draw_codebooks(key, part):
    return book_table(key)


def draw_query_embed(key, part):
    base = jax.random.fold_in(key, 7005)
    first = jax.random.fold_in(base, 0)
    values = jnp.clip(jax.random.normal(first, (N_BLK, N_REP, QR, E), jnp.float32) * 2.0, -12.0, 12.0)
    return values.astype(jnp.bfloat16)


def setup_inputs(seed: int = 0) -> dict:
    seeds = jax.random.split(jax.random.key(seed), 6)
    return {
        "query_embed": draw_query_embed(jax.random.fold_in(seeds[5], 71), 0),
        "positive_ids": draw_positive_ids(jax.random.fold_in(seeds[5], 71), 0),
        "pair_blocks": draw_pair_blocks(jax.random.fold_in(seeds[5], 71), 0),
        "code_ids": draw_code_ids(jax.random.fold_in(seeds[5], 71), 0),
        "codebooks": draw_codebooks(jax.random.fold_in(seeds[5], 71), 0),
    }


EPS = 1e-06

def reference(query_embed, positive_ids, pair_blocks, code_ids, codebooks):
    block_count, rep_count, query_rows, feat_count = query_embed.shape
    block_rows = PR * rep_count
    pair_count = pair_blocks.shape[1]
    table = codebooks.astype(jnp.float32)
    quant = jnp.zeros((block_count, rep_count, PBLK_DEV * PR, feat_count), jnp.float32)
    for book_index in range(BOOKS):
        quant = quant + table[code_ids[:, :, book_index, :] + book_index * CODES]
    inverse = lax.rsqrt(lax.optimization_barrier(jnp.sum(quant * quant, axis=-1, keepdims=True)) + EPS)
    unit = quant * inverse
    unit_bf = unit.astype(jnp.bfloat16)
    blocks = unit_bf.reshape(block_count, rep_count, PBLK_DEV, PR, feat_count)
    blocks = blocks.transpose(0, 2, 1, 3, 4).reshape(block_count * PBLK_DEV, block_rows, feat_count)
    column_ids = jnp.arange(pair_count * block_rows, dtype=jnp.int32)
    slot_ids = jnp.arange(pair_count, dtype=jnp.int32)

    def one_block(carry, item):
        row_block, targets, chosen = item
        columns = blocks[chosen].reshape(pair_count * block_rows, feat_count)
        scores = jnp.dot(row_block, columns.T, preferred_element_type=jnp.float32)
        peak = lax.optimization_barrier(jnp.max(scores, axis=1, keepdims=True))
        lse = peak[:, 0] + jnp.log(lax.optimization_barrier(jnp.sum(jnp.exp(scores - peak), axis=1)))
        target_block = targets // block_rows
        target_slot = lax.optimization_barrier(jnp.sum(jnp.where(chosen[None, :] == target_block[:, None], slot_ids[None, :], 0), axis=1)).astype(jnp.int32)
        target_col = target_slot * block_rows + targets % block_rows
        hit_mask = column_ids[None, :] == target_col[:, None]
        target = lax.optimization_barrier(jnp.sum(jnp.where(hit_mask, scores, 0.0), axis=1))
        weight = (jnp.exp(scores - lse[:, None]) - hit_mask.astype(jnp.float32)).astype(jnp.bfloat16)
        grad_rows = jnp.dot(weight, columns, preferred_element_type=jnp.float32)
        grad_cols = jnp.dot(weight.T, row_block, preferred_element_type=jnp.float32)
        carry = carry.at[chosen].add(grad_cols.reshape(pair_count, block_rows, feat_count))
        return (carry, (lse - target, grad_rows))
    start = jnp.zeros((block_count * PBLK_DEV, block_rows, feat_count), jnp.float32)
    inputs = (query_embed.reshape(block_count, rep_count * query_rows, feat_count), positive_ids.reshape(block_count, rep_count * query_rows), pair_blocks)
    unit_grad, (losses, grads) = lax.scan(one_block, start, inputs)
    unit_grad = unit_grad.reshape(block_count, PBLK_DEV, rep_count, PR, feat_count)
    unit_grad = unit_grad.transpose(0, 2, 1, 3, 4).reshape(block_count, rep_count, PBLK_DEV * PR, feat_count)
    passage_grad = inverse * (unit_grad - unit * lax.optimization_barrier(jnp.sum(unit * unit_grad, axis=-1, keepdims=True)))
    flat_grad = passage_grad.reshape(-1, feat_count)
    pieces = []
    for book_index in range(BOOKS):
        members = code_ids[:, :, book_index, :].reshape(-1)
        pieces.append(jax.ops.segment_sum(flat_grad, members, num_segments=CODES))
    codebook_grad = jnp.concatenate(pieces, axis=0)
    query_loss = losses.reshape(block_count, rep_count, query_rows)
    query_grad = grads.reshape(block_count, rep_count, query_rows, feat_count)
    return (query_loss, query_grad, passage_grad, codebook_grad)
```

```python
import functools

import jax
import jax.numpy as jnp
from jax import lax
from jax.experimental import pallas as pl
from jax.experimental.pallas import tpu as pltpu
from jax.sharding import PartitionSpec as P

CODES = 256
PR = 16
PBLK_DEV = 4
LANES = 128
SUBS = 8
EPS = 1e-06
F32 = jnp.float32
BF16 = jnp.bfloat16
MESH = pl.DeviceIdType.MESH


def log2(n):
    assert n & (n - 1) == 0
    return n.bit_length() - 1


def div(x, n):
    return lax.shift_right_logical(x, jnp.int32(log2(n)))


def mod(x, n):
    return x & (n - 1)


def iota(shape, dim):
    return lax.broadcasted_iota(jnp.int32, shape, dim)


def dot(a, b, dims=((1,), (0,))):
    return lax.dot_general(a, b, (dims, ((), ())), preferred_element_type=F32)


def loop(count, body):
    if count <= 8:
        for k in range(count):
            body(k)
    else:

        def step(k, carry):
            body(k)
            return carry

        lax.fori_loop(0, count, step, 0)


def kernel(
    nb, nr, pairs,
    q_ref, pos_ref, pair_ref, code_ref, book_ref,
    loss_ref, qgrad_ref, pgrad_ref, cgrad_ref,
    info, pair_unit, own_unit, own_inv, own_codes, send2, recv2, sums, blocks, total, send4, recv4,
    info_send, info_recv, s2, r2, s3, f3, r3, s4, r4,
):
    me_b = lax.axis_index("blk")
    me_r = lax.axis_index("rep")
    me = me_b * nr + me_r
    nd = nb * nr
    books = code_ref.shape[0]
    feat = q_ref.shape[1]
    rows = q_ref.shape[0]
    span = pairs * PR
    own_rows = PBLK_DEV * PR

    codes = code_ref[...].astype(F32).astype(BF16)
    lane = iota((own_rows, LANES), 1)
    sub = iota((own_rows, LANES), 0)
    keep = iota((books, LANES), 0) == div(iota((books, LANES), 1), PR)
    sub8 = iota((SUBS, LANES), 0)
    mine = jnp.zeros((SUBS, LANES), F32)
    for j in range(PBLK_DEV):
        shift = (sub == j * PR + mod(lane, PR)).astype(BF16)
        line = jnp.sum(jnp.where(keep, dot(codes, shift), 0.0), axis=0, keepdims=True)
        mine = jnp.where(sub8 == j, line, mine)
    spread = (iota((pairs, LANES), 0) == iota((pairs, LANES), 1)).astype(BF16)
    pair_line = dot(jnp.broadcast_to(pair_ref[...].astype(F32), (SUBS, pairs)).astype(BF16), spread)
    mine = jnp.where(sub8 == PBLK_DEV, pair_line, mine)
    info[me] = mine

    def tell(k, carry):
        to = lax.rem(me + k, nd)
        pltpu.make_async_remote_copy(
            src_ref=info.at[me], dst_ref=info.at[me],
            send_sem=info_send, recv_sem=info_recv,
            device_id={"blk": to // nr, "rep": lax.rem(to, nr)}, device_id_type=MESH,
        ).start()
        return carry

    lax.fori_loop(1, nd, tell, 0)
    everyone = info.at[pl.ds(0, nd - 1)]
    pltpu.make_async_copy(everyone, everyone, info_recv).wait()

    heard = info[...].reshape(nd * SUBS, LANES).astype(BF16)
    chunk = min(32, nb * PBLK_DEV, nr * pairs)
    tall = chunk * PR
    pair_row = mine[PBLK_DEV : PBLK_DEV + 1, :]
    grow = (div(iota((tall, chunk), 0), PR) == iota((tall, chunk), 1)).astype(BF16)
    in_row = mod(iota((tall, LANES), 0), PR) == mod(iota((tall, LANES), 1), PR)
    code_line = iota((1, CODES), 1).astype(F32)
    wide = iota((chunk, nd * SUBS), 1)
    from_dev = div(wide, SUBS)
    from_row = mod(wide, SUBS)

    def code_of(spread_codes, book):
        pick = (div(iota((LANES, CODES), 0), PR) == book).astype(BF16)
        return dot(spread_codes, pick)

    def embed(select):
        picked = dot(select.astype(BF16), heard)
        spread_codes = jnp.where(in_row, dot(grow, picked.astype(BF16)), 0.0).astype(BF16)
        quant = jnp.zeros((tall, feat), F32)
        for k in range(books):
            onehot = (code_of(spread_codes, k) == code_line).astype(BF16)
            quant = quant + dot(onehot, book_ref[pl.ds(k * CODES, CODES), :])
        inverse = lax.rsqrt(jnp.sum(quant * quant, axis=1, keepdims=True) + EPS)
        return spread_codes, quant * inverse, inverse

    def pair_chunk(c):
        row = iota((chunk, 1), 0) + c * chunk
        slot = mod(row, pairs)
        rep = div(row, pairs)
        block = jnp.sum(
            jnp.where(iota((chunk, LANES), 1) == slot, pair_row, 0.0), axis=1, keepdims=True
        ).astype(jnp.int32)
        select = (
            (div(from_dev, nr) * PBLK_DEV + from_row == block)
            & (from_row < PBLK_DEV)
            & (mod(from_dev, nr) == rep)
        )
        unused, unit, inverse = embed(select)
        pair_unit[pl.ds(c * tall, tall), :] = unit.astype(BF16)

    loop(nr * pairs // chunk, pair_chunk)

    repeat = (iota((LANES, span), 0) == div(iota((LANES, span), 1), PR)).astype(BF16)
    my_blocks = dot(jnp.broadcast_to(pair_row, (SUBS, LANES)).astype(BF16), repeat)[0:1, :]
    inner = mod(iota((1, span), 1), PR).astype(F32)
    column_ids = jnp.concatenate(
        [my_blocks * (PR * nr) + (inner + r * PR) for r in range(nr)], axis=1
    )
    eye = iota((rows, rows), 0) == iota((rows, rows), 1)
    goal = jnp.sum(
        jnp.where(eye, pos_ref[pl.ds(me_r, 1), :].astype(F32), 0.0), axis=1, keepdims=True
    )
    query = q_ref[...]
    unit_bf = pair_unit[...]
    scores = dot(query, unit_bf, ((1,), (1,)))
    hit = column_ids == goal
    peak = jnp.max(scores, axis=1, keepdims=True)
    lse = peak + jnp.log(jnp.sum(jnp.exp(scores - peak), axis=1, keepdims=True))
    target = jnp.sum(jnp.where(hit, scores, 0.0), axis=1, keepdims=True)
    weight = (jnp.exp(scores - lse) - hit.astype(F32)).astype(BF16)
    grad_cols = dot(weight, query, ((0,), (0,)))
    send2[...] = grad_cols.astype(BF16).reshape(nr, span, feat)
    moves2 = []
    for d in range(nr - 1, 0, -1):
        to = lax.rem(me_r + d, nr)
        move = pltpu.make_async_remote_copy(
            src_ref=send2.at[to], dst_ref=recv2.at[d], send_sem=s2.at[d], recv_sem=r2.at[d],
            device_id={"blk": me_b, "rep": to}, device_id_type=MESH,
        )
        move.start()
        moves2.append(move)
    loss_ref[...] = jnp.sum(jnp.where(eye, lse - target, 0.0), axis=0, keepdims=True)
    qgrad_ref[...] = dot(weight, unit_bf)

    def own_chunk(c):
        row = iota((chunk, 1), 0) + c * chunk
        select = (from_dev == div(row, PBLK_DEV) * nr + me_r) & (from_row == mod(row, PBLK_DEV))
        spread_codes, unit, inverse = embed(select)
        own_unit[pl.ds(c * tall, tall), :] = unit
        own_inv[pl.ds(c * tall, tall), :] = jnp.broadcast_to(inverse, (tall, LANES))
        own_codes[pl.ds(c * tall, tall), :] = spread_codes

    loop(nb * PBLK_DEV // chunk, own_chunk)
    directory = jnp.concatenate(
        [info[b * nr][PBLK_DEV : PBLK_DEV + 1, :] for b in range(nb)], axis=0
    )
    blocks[...] = dot(directory.astype(BF16), repeat)

    for move in moves2:
        move.wait()
    summed = send2[me_r].astype(F32)
    for d in range(1, nr):
        summed = summed + recv2[d].astype(F32)
    sums[me_b] = summed.astype(BF16)

    peer = me_b + 1 - 2 * lax.rem(me_b, 2)
    half = nb // 2

    def share(slot, to, send_sem):
        return pltpu.make_async_remote_copy(
            src_ref=sums.at[slot], dst_ref=sums.at[slot], send_sem=send_sem,
            recv_sem=r3.at[slot], device_id={"blk": to, "rep": me_r}, device_id_type=MESH,
        )

    def add_block(b):
        line = blocks[pl.ds(b, 1), :].astype(jnp.int32)
        part = sums[b]

        def rows_chunk(c):
            row = iota((tall, span), 0) + c * tall
            select = (div(row, PR) == line) & (mod(row, PR) == mod(iota((tall, span), 1), PR))
            total[pl.ds(c * tall, tall), :] += dot(select.astype(BF16), part)

        loop(nb * PBLK_DEV // chunk, rows_chunk)

    share(me_b, peer, s3.at[0]).start()
    loop(half - 1, lambda k: share(me_b, lax.rem(me_b + 2 * (k + 1), nb), s3.at[k + 1]).start())
    total[...] = jnp.zeros_like(total)
    add_block(me_b)

    def pass_on(k):
        slot = lax.rem(me_b + nb - 2 * (k + 1), nb)
        share(slot, peer, f3.at[k]).wait_recv()
        share(slot, peer, f3.at[k]).start()
        add_block(slot)

    loop(half - 1, pass_on)

    def take(k):
        slot = lax.rem(peer + nb - 2 * k, nb)
        share(slot, peer, s3.at[0]).wait_recv()
        add_block(slot)

    loop(half, take)

    unit = own_unit[...]
    grad = total[...]
    grad = own_inv[:, 0:1] * (grad - unit * jnp.sum(unit * grad, axis=1, keepdims=True))
    total[...] = grad
    pgrad_ref[...] = total[pl.ds(me_b * own_rows, own_rows), :]

    group = send4.shape[0] * send4.shape[1]
    first = me_b * group
    wanted = code_of(own_codes[...], first // CODES)[:, 0:group]
    member = wanted == (iota((1, group), 1) + lax.rem(first, CODES)).astype(F32)
    part = dot(member.astype(BF16), grad.astype(BF16), ((0,), (0,)))
    send4[...] = part.astype(BF16).reshape(send4.shape)
    moves4 = []
    for d in range(nr - 1, 0, -1):
        to = lax.rem(me_r + d, nr)
        move = pltpu.make_async_remote_copy(
            src_ref=send4.at[to], dst_ref=recv4.at[d], send_sem=s4.at[d], recv_sem=r4.at[d],
            device_id={"blk": me_b, "rep": to}, device_id_type=MESH,
        )
        move.start()
        moves4.append(move)
    pltpu.make_async_copy(everyone, everyone, info_send).wait()
    loop(half, lambda k: share(me_b, peer, s3.at[k]).wait_send())
    loop(half - 1, lambda k: share(me_b, peer, f3.at[k]).wait_send())
    for move in moves4:
        move.wait()
    summed = send4[me_r].astype(F32)
    for d in range(1, nr):
        summed = summed + recv4[d].astype(F32)
    cgrad_ref[...] = summed


def shards(query_embed, positive_ids, pair_blocks, code_ids, codebooks):
    nb = lax.axis_size("blk")
    nr = lax.axis_size("rep")
    rows, feat = query_embed.shape[2:]
    pairs = pair_blocks.shape[1]
    books = code_ids.shape[2]
    share_rows = codebooks.shape[0] // (nb * nr)
    span = pairs * PR
    passages = nb * PBLK_DEV * PR
    assert books * PR == LANES and codebooks.shape[0] == books * CODES and pairs <= LANES
    assert CODES % (share_rows * nr) == 0 and nb * PBLK_DEV <= 256 and CODES <= 256
    vmem = pl.BlockSpec(memory_space=pltpu.VMEM)
    dma = pltpu.SemaphoreType.DMA
    outs = pl.pallas_call(
        functools.partial(kernel, nb, nr, pairs),
        out_shape=(
            jax.ShapeDtypeStruct((1, rows), F32),
            jax.ShapeDtypeStruct((rows, feat), F32),
            jax.ShapeDtypeStruct((PBLK_DEV * PR, feat), F32),
            jax.ShapeDtypeStruct((share_rows, feat), F32),
        ),
        in_specs=[vmem] * 5,
        out_specs=(vmem,) * 4,
        scratch_shapes=[
            pltpu.VMEM((nb * nr, SUBS, LANES), F32),
            pltpu.VMEM((nr * span, feat), BF16),
            pltpu.VMEM((passages, feat), F32),
            pltpu.VMEM((passages, LANES), F32),
            pltpu.VMEM((passages, LANES), BF16),
            pltpu.VMEM((nr, span, feat), BF16),
            pltpu.VMEM((nr, span, feat), BF16),
            pltpu.VMEM((nb, span, feat), BF16),
            pltpu.VMEM((nb, span), F32),
            pltpu.VMEM((passages, feat), F32),
            pltpu.VMEM((nr, share_rows, feat), BF16),
            pltpu.VMEM((nr, share_rows, feat), BF16),
            dma, dma, dma((nr,)), dma((nr,)),
            dma((nb // 2,)), dma((nb // 2,)), dma((nb,)), dma((nr,)), dma((nr,)),
        ],
        compiler_params=pltpu.CompilerParams(
            has_side_effects=True, vmem_limit_bytes=67_000_000
        ),
    )(query_embed[0, 0], positive_ids[0], pair_blocks, code_ids[0, 0], codebooks)
    loss, query_grad, passage_grad, codebook_grad = outs
    return (loss[None], query_grad[None, None], passage_grad[None, None], codebook_grad)


def solution(mesh):
    placed = (
        P("blk", "rep", None, None),
        P("blk", None, None),
        P("blk", None),
        P("blk", "rep", None, None),
        P(),
    )
    return jax.shard_map(
        shards,
        mesh=mesh,
        in_specs=placed,
        out_specs=(
            P("blk", "rep", None),
            P("blk", "rep", None, None),
            P("blk", "rep", None, None),
            P(("blk", "rep"), None),
        ),
        check_vma=False,
    )
```

```python
import functools

import jax
import jax.numpy as jnp
from jax import lax
from jax.experimental import pallas as pl
from jax.experimental.pallas import tpu as pltpu
from jax.sharding import PartitionSpec as P

CODES = 256
PR = 16
PBLK_DEV = 4
LANES = 128
SUBS = 8
EPS = 1e-06
F32 = jnp.float32
BF16 = jnp.bfloat16
MESH = pl.DeviceIdType.MESH


def log2(n):
    assert n & (n - 1) == 0
    return n.bit_length() - 1


def div(x, n):
    return lax.shift_right_logical(x, jnp.int32(log2(n)))


def mod(x, n):
    return x & (n - 1)


def iota(shape, dim):
    return lax.broadcasted_iota(jnp.int32, shape, dim)


def dot(a, b, dims=((1,), (0,))):
    return lax.dot_general(a, b, (dims, ((), ())), preferred_element_type=F32)


def loop(count, body):
    if count <= 8:
        for k in range(count):
            body(k)
    else:

        def step(k, carry):
            body(k)
            return carry

        lax.fori_loop(0, count, step, 0)


def kernel(
    nb, nr, pairs,
    q_ref, pos_ref, pair_ref, code_ref, book_ref,
    loss_ref, qgrad_ref, pgrad_ref, cgrad_ref,
    info, pair_unit, own_unit, own_inv, own_codes, send2, recv2, sums, blocks, total, send4, recv4,
    blk_send, blk_recv, rep_send, rep_recv, s2, r2, s3, f3, r3, s4, r4,
):
    me_b = lax.axis_index("blk")
    me_r = lax.axis_index("rep")
    barrier = pltpu.get_barrier_semaphore()
    for d in range(1, nr):
        pl.semaphore_signal(
            barrier, inc=1, device_id={"blk": me_b, "rep": lax.rem(me_r + d, nr)},
            device_id_type=MESH,
        )
    loop(
        nb - 1,
        lambda k: pl.semaphore_signal(
            barrier, inc=1, device_id={"blk": lax.rem(me_b + k + 1, nb), "rep": me_r},
            device_id_type=MESH,
        ),
    )
    books = code_ref.shape[0]
    feat = q_ref.shape[1]
    rows = q_ref.shape[0]
    span = pairs * PR
    own_rows = PBLK_DEV * PR

    codes = code_ref[...].astype(F32).astype(BF16)
    lane = iota((own_rows, LANES), 1)
    sub = iota((own_rows, LANES), 0)
    keep = iota((books, LANES), 0) == div(iota((books, LANES), 1), PR)
    sub8 = iota((SUBS, LANES), 0)
    mine = jnp.zeros((SUBS, LANES), F32)
    for j in range(PBLK_DEV):
        shift = (sub == j * PR + mod(lane, PR)).astype(BF16)
        line = jnp.sum(jnp.where(keep, dot(codes, shift), 0.0), axis=0, keepdims=True)
        mine = jnp.where(sub8 == j, line, mine)
    spread = (iota((pairs, LANES), 0) == iota((pairs, LANES), 1)).astype(BF16)
    pair_line = dot(jnp.broadcast_to(pair_ref[...].astype(F32), (SUBS, pairs)).astype(BF16), spread)
    mine = jnp.where(sub8 == PBLK_DEV, pair_line, mine)
    info[me_r, me_b] = mine
    pl.semaphore_wait(barrier, nr - 1 + nb - 1)

    def tell_blk(to):
        return pltpu.make_async_remote_copy(
            src_ref=info.at[me_r, me_b], dst_ref=info.at[me_r, me_b],
            send_sem=blk_send, recv_sem=blk_recv,
            device_id={"blk": to, "rep": me_r}, device_id_type=MESH,
        )

    def tell_rep(to):
        return pltpu.make_async_remote_copy(
            src_ref=info.at[me_r], dst_ref=info.at[me_r],
            send_sem=rep_send, recv_sem=rep_recv,
            device_id={"blk": me_b, "rep": to}, device_id_type=MESH,
        )

    loop(nb - 1, lambda k: tell_blk(lax.rem(me_b + k + 1, nb)).start())
    others_blk = info.at[0, pl.ds(0, nb - 1)]
    others_rep = info.at[pl.ds(0, nr - 1)]
    pltpu.make_async_copy(others_blk, others_blk, blk_recv).wait()
    for d in range(nr - 1, 0, -1):
        tell_rep(lax.rem(me_r + d, nr)).start()

    chunk = min(32, nb * PBLK_DEV, nr * pairs)
    flat = nb * SUBS
    tall = chunk * PR
    pair_row = mine[PBLK_DEV : PBLK_DEV + 1, :]
    grow = (div(iota((tall, chunk), 0), PR) == iota((tall, chunk), 1)).astype(BF16)
    in_row = mod(iota((tall, LANES), 0), PR) == mod(iota((tall, LANES), 1), PR)
    code_line = iota((1, CODES), 1).astype(F32)
    def code_of(spread_codes, book):
        pick = (div(iota((LANES, CODES), 0), PR) == book).astype(BF16)
        return dot(spread_codes, pick)

    def embed(select, heard):
        picked = dot(select.astype(BF16), heard)
        spread_codes = jnp.where(in_row, dot(grow, picked.astype(BF16)), 0.0).astype(BF16)
        quant = jnp.zeros((tall, feat), F32)
        for k in range(books):
            onehot = (code_of(spread_codes, k) == code_line).astype(BF16)
            quant = quant + dot(onehot, book_ref[pl.ds(k * CODES, CODES), :])
        inverse = lax.rsqrt(jnp.sum(quant * quant, axis=1, keepdims=True) + EPS)
        return spread_codes, quant * inverse, inverse

    heard_own = info[me_r].reshape(flat, LANES).astype(BF16)

    def own_chunk(c):
        row = iota((chunk, 1), 0) + c * chunk
        wide = iota((chunk, flat), 1)
        select = (div(wide, SUBS) == div(row, PBLK_DEV)) & (mod(wide, SUBS) == mod(row, PBLK_DEV))
        spread_codes, unit, inverse = embed(select, heard_own)
        own_unit[pl.ds(c * tall, tall), :] = unit
        own_inv[pl.ds(c * tall, tall), :] = jnp.broadcast_to(inverse, (tall, LANES))
        own_codes[pl.ds(c * tall, tall), :] = spread_codes

    loop(nb * PBLK_DEV // chunk, own_chunk)
    repeat = (iota((LANES, span), 0) == div(iota((LANES, span), 1), PR)).astype(BF16)
    directory = jnp.concatenate(
        [info[me_r, b][PBLK_DEV : PBLK_DEV + 1, :] for b in range(nb)], axis=0
    )
    blocks[...] = dot(directory.astype(BF16), repeat)

    pltpu.make_async_copy(others_rep, others_rep, rep_recv).wait()
    heard = info[...].reshape(nr * flat, LANES).astype(BF16)
    wide = iota((chunk, nr * flat), 1)
    from_dev = div(wide, SUBS)
    from_row = mod(wide, SUBS)

    def pair_chunk(c):
        row = iota((chunk, 1), 0) + c * chunk
        slot = mod(row, pairs)
        rep = div(row, pairs)
        block = jnp.sum(
            jnp.where(iota((chunk, LANES), 1) == slot, pair_row, 0.0), axis=1, keepdims=True
        ).astype(jnp.int32)
        select = (
            (mod(from_dev, nb) * PBLK_DEV + from_row == block)
            & (from_row < PBLK_DEV)
            & (div(from_dev, nb) == rep)
        )
        unused, unit, inverse = embed(select, heard)
        pair_unit[pl.ds(c * tall, tall), :] = unit.astype(BF16)

    loop(nr * pairs // chunk, pair_chunk)

    my_blocks = dot(jnp.broadcast_to(pair_row, (SUBS, LANES)).astype(BF16), repeat)[0:1, :]
    inner = mod(iota((1, span), 1), PR).astype(F32)
    column_ids = jnp.concatenate(
        [my_blocks * (PR * nr) + (inner + r * PR) for r in range(nr)], axis=1
    )
    eye = iota((rows, rows), 0) == iota((rows, rows), 1)
    goal = jnp.sum(
        jnp.where(eye, pos_ref[pl.ds(me_r, 1), :].astype(F32), 0.0), axis=1, keepdims=True
    )
    query = q_ref[...]
    unit_bf = pair_unit[...]
    scores = dot(query, unit_bf, ((1,), (1,)))
    hit = column_ids == goal
    peak = jnp.max(scores, axis=1, keepdims=True)
    lse = peak + jnp.log(jnp.sum(jnp.exp(scores - peak), axis=1, keepdims=True))
    target = jnp.sum(jnp.where(hit, scores, 0.0), axis=1, keepdims=True)
    weight = (jnp.exp(scores - lse) - hit.astype(F32)).astype(BF16)
    grad_cols = dot(weight, query, ((0,), (0,)))
    send2[...] = grad_cols.astype(BF16).reshape(nr, span, feat)
    moves2 = []
    for d in range(nr - 1, 0, -1):
        to = lax.rem(me_r + d, nr)
        move = pltpu.make_async_remote_copy(
            src_ref=send2.at[to], dst_ref=recv2.at[d], send_sem=s2.at[d], recv_sem=r2.at[d],
            device_id={"blk": me_b, "rep": to}, device_id_type=MESH,
        )
        move.start()
        moves2.append(move)
    loss_ref[...] = jnp.sum(jnp.where(eye, lse - target, 0.0), axis=0, keepdims=True)
    qgrad_ref[...] = dot(weight, unit_bf)

    for move in moves2:
        move.wait()
    summed = send2[me_r].astype(F32)
    for d in range(1, nr):
        summed = summed + recv2[d].astype(F32)
    sums[me_b] = summed.astype(BF16)

    peer = me_b + 1 - 2 * lax.rem(me_b, 2)
    half = nb // 2

    def share(slot, to, send_sem):
        return pltpu.make_async_remote_copy(
            src_ref=sums.at[slot], dst_ref=sums.at[slot], send_sem=send_sem,
            recv_sem=r3.at[slot], device_id={"blk": to, "rep": me_r}, device_id_type=MESH,
        )

    def add_block(b):
        line = blocks[pl.ds(b, 1), :].astype(jnp.int32)
        part = sums[b]

        def rows_chunk(c):
            row = iota((tall, span), 0) + c * tall
            select = (div(row, PR) == line) & (mod(row, PR) == mod(iota((tall, span), 1), PR))
            total[pl.ds(c * tall, tall), :] += dot(select.astype(BF16), part)

        loop(nb * PBLK_DEV // chunk, rows_chunk)

    share(me_b, peer, s3.at[0]).start()
    loop(half - 1, lambda k: share(me_b, lax.rem(me_b + 2 * (k + 1), nb), s3.at[k + 1]).start())
    total[...] = jnp.zeros_like(total)
    add_block(me_b)

    def pass_on(k):
        slot = lax.rem(me_b + nb - 2 * (k + 1), nb)
        share(slot, peer, f3.at[k]).wait_recv()
        share(slot, peer, f3.at[k]).start()
        add_block(slot)

    loop(half - 1, pass_on)

    def take(k):
        slot = lax.rem(peer + nb - 2 * k, nb)
        share(slot, peer, s3.at[0]).wait_recv()
        add_block(slot)

    loop(half, take)

    unit = own_unit[...]
    grad = total[...]
    grad = own_inv[:, 0:1] * (grad - unit * jnp.sum(unit * grad, axis=1, keepdims=True))
    total[...] = grad
    pgrad_ref[...] = total[pl.ds(me_b * own_rows, own_rows), :]

    group = send4.shape[0] * send4.shape[1]
    first = me_b * group
    wanted = code_of(own_codes[...], first // CODES)[:, 0:group]
    member = wanted == (iota((1, group), 1) + lax.rem(first, CODES)).astype(F32)
    part = dot(member.astype(BF16), grad.astype(BF16), ((0,), (0,)))
    send4[...] = part.astype(BF16).reshape(send4.shape)
    moves4 = []
    for d in range(nr - 1, 0, -1):
        to = lax.rem(me_r + d, nr)
        move = pltpu.make_async_remote_copy(
            src_ref=send4.at[to], dst_ref=recv4.at[d], send_sem=s4.at[d], recv_sem=r4.at[d],
            device_id={"blk": me_b, "rep": to}, device_id_type=MESH,
        )
        move.start()
        moves4.append(move)
    pltpu.make_async_copy(others_blk, others_blk, blk_send).wait()
    pltpu.make_async_copy(others_rep, others_rep, rep_send).wait()
    loop(half, lambda k: share(me_b, peer, s3.at[k]).wait_send())
    loop(half - 1, lambda k: share(me_b, peer, f3.at[k]).wait_send())
    for move in moves4:
        move.wait()
    summed = send4[me_r].astype(F32)
    for d in range(1, nr):
        summed = summed + recv4[d].astype(F32)
    cgrad_ref[...] = summed


def write_out(*refs):
    sems = refs[8]
    moves = [pltpu.make_async_copy(refs[k], refs[k + 4], sems.at[k]) for k in range(4)]
    for move in moves:
        move.start()
    for move in moves:
        move.wait()


def shards(query_embed, positive_ids, pair_blocks, code_ids, codebooks):
    nb = lax.axis_size("blk")
    nr = lax.axis_size("rep")
    rows, feat = query_embed.shape[2:]
    pairs = pair_blocks.shape[1]
    books = code_ids.shape[2]
    share_rows = codebooks.shape[0] // (nb * nr)
    span = pairs * PR
    passages = nb * PBLK_DEV * PR
    assert books * PR == LANES and codebooks.shape[0] == books * CODES and pairs <= LANES
    assert CODES % (share_rows * nr) == 0 and nb * PBLK_DEV <= 256 and CODES <= 256
    vmem = pl.BlockSpec(memory_space=pltpu.VMEM)
    hbm = pl.BlockSpec(memory_space=pltpu.HBM)
    dma = pltpu.SemaphoreType.DMA
    limit = 67_000_000 if nb * span * feat > 8_000_000 else 32_000_000
    shapes = (
        jax.ShapeDtypeStruct((1, rows), F32),
        jax.ShapeDtypeStruct((rows, feat), F32),
        jax.ShapeDtypeStruct((PBLK_DEV * PR, feat), F32),
        jax.ShapeDtypeStruct((share_rows, feat), F32),
    )
    outs = pl.pallas_call(
        functools.partial(kernel, nb, nr, pairs),
        out_shape=shapes,
        in_specs=[vmem] * 5,
        out_specs=(vmem,) * 4,
        scratch_shapes=[
            pltpu.VMEM((nr, nb, SUBS, LANES), F32),
            pltpu.VMEM((nr * span, feat), BF16),
            pltpu.VMEM((passages, feat), F32),
            pltpu.VMEM((passages, LANES), F32),
            pltpu.VMEM((passages, LANES), BF16),
            pltpu.VMEM((nr, span, feat), BF16),
            pltpu.VMEM((nr, span, feat), BF16),
            pltpu.VMEM((nb, span, feat), BF16),
            pltpu.VMEM((nb, span), F32),
            pltpu.VMEM((passages, feat), F32),
            pltpu.VMEM((nr, share_rows, feat), BF16),
            pltpu.VMEM((nr, share_rows, feat), BF16),
            dma, dma, dma, dma, dma((nr,)), dma((nr,)),
            dma((nb // 2,)), dma((nb // 2,)), dma((nb,)), dma((nr,)), dma((nr,)),
        ],
        compiler_params=pltpu.CompilerParams(
            has_side_effects=True, collective_id=0, vmem_limit_bytes=limit
        ),
    )(query_embed[0, 0], positive_ids[0], pair_blocks, code_ids[0, 0], codebooks)
    loss, query_grad, passage_grad, codebook_grad = pl.pallas_call(
        write_out,
        out_shape=shapes,
        in_specs=[vmem] * 4,
        out_specs=(hbm,) * 4,
        scratch_shapes=[dma((4,))],
        compiler_params=pltpu.CompilerParams(vmem_limit_bytes=8_000_000),
    )(*outs)
    return (loss[None], query_grad[None, None], passage_grad[None, None], codebook_grad)


def solution(mesh):
    placed = (
        P("blk", "rep", None, None),
        P("blk", None, None),
        P("blk", None),
        P("blk", "rep", None, None),
        P(),
    )
    return jax.shard_map(
        shards,
        mesh=mesh,
        in_specs=placed,
        out_specs=(
            P("blk", "rep", None),
            P("blk", "rep", None, None),
            P("blk", "rep", None, None),
            P(("blk", "rep"), None),
        ),
        check_vma=False,
    )
```

```python
import functools

import jax
import jax.numpy as jnp
from jax import lax
from jax.experimental import pallas as pl
from jax.experimental.pallas import tpu as pltpu
from jax.sharding import PartitionSpec as P

CODES = 256
PR = 16
PBLK_DEV = 4
LANES = 128
SUBS = 8
PARTS = 2
EPS = 1e-06
F32 = jnp.float32
BF16 = jnp.bfloat16
MESH = pl.DeviceIdType.MESH


def log2(n):
    assert n & (n - 1) == 0
    return n.bit_length() - 1


def div(x, n):
    return lax.shift_right_logical(x, jnp.int32(log2(n)))


def mod(x, n):
    return x & (n - 1)


def iota(shape, dim):
    return lax.broadcasted_iota(jnp.int32, shape, dim)


def dot(a, b, dims=((1,), (0,))):
    return lax.dot_general(a, b, (dims, ((), ())), preferred_element_type=F32)


def loop(count, body):
    if count <= 8:
        for k in range(count):
            body(k)
    else:

        def step(k, carry):
            body(k)
            return carry

        lax.fori_loop(0, count, step, 0)


def kernel(
    nb, nr, pairs,
    q_ref, pos_ref, pair_ref, code_ref, book_ref,
    loss_ref, qgrad_ref, pgrad_ref, cgrad_ref,
    info, pair_unit, own_unit, own_inv, own_codes, send2, recv2, sums, blocks, total, send4, recv4,
    blk_send, blk_recv, rep_send, rep_recv, s2, r2, s3, f3, r3, s4, r4,
):
    me_b = lax.axis_index("blk")
    me_r = lax.axis_index("rep")
    barrier = pltpu.get_barrier_semaphore()
    for d in range(1, nr):
        pl.semaphore_signal(
            barrier, inc=1, device_id={"blk": me_b, "rep": lax.rem(me_r + d, nr)},
            device_id_type=MESH,
        )
    loop(
        nb - 1,
        lambda k: pl.semaphore_signal(
            barrier, inc=1, device_id={"blk": lax.rem(me_b + k + 1, nb), "rep": me_r},
            device_id_type=MESH,
        ),
    )
    books = code_ref.shape[0]
    feat = q_ref.shape[1]
    rows = q_ref.shape[0]
    span = pairs * PR
    own_rows = PBLK_DEV * PR

    codes = code_ref[...].astype(F32).astype(BF16)
    lane = iota((own_rows, LANES), 1)
    sub = iota((own_rows, LANES), 0)
    keep = iota((books, LANES), 0) == div(iota((books, LANES), 1), PR)
    sub8 = iota((SUBS, LANES), 0)
    mine = jnp.zeros((SUBS, LANES), F32)
    for j in range(PBLK_DEV):
        shift = (sub == j * PR + mod(lane, PR)).astype(BF16)
        line = jnp.sum(jnp.where(keep, dot(codes, shift), 0.0), axis=0, keepdims=True)
        mine = jnp.where(sub8 == j, line, mine)
    spread = (iota((pairs, LANES), 0) == iota((pairs, LANES), 1)).astype(BF16)
    pair_line = dot(jnp.broadcast_to(pair_ref[...].astype(F32), (SUBS, pairs)).astype(BF16), spread)
    mine = jnp.where(sub8 == PBLK_DEV, pair_line, mine)
    info[me_r, me_b] = mine
    pl.semaphore_wait(barrier, nr - 1 + nb - 1)

    def tell_blk(to):
        return pltpu.make_async_remote_copy(
            src_ref=info.at[me_r, me_b], dst_ref=info.at[me_r, me_b],
            send_sem=blk_send, recv_sem=blk_recv,
            device_id={"blk": to, "rep": me_r}, device_id_type=MESH,
        )

    def tell_rep(to):
        return pltpu.make_async_remote_copy(
            src_ref=info.at[me_r], dst_ref=info.at[me_r],
            send_sem=rep_send, recv_sem=rep_recv,
            device_id={"blk": me_b, "rep": to}, device_id_type=MESH,
        )

    loop(nb - 1, lambda k: tell_blk(lax.rem(me_b + k + 1, nb)).start())
    others_blk = info.at[0, pl.ds(0, nb - 1)]
    others_rep = info.at[pl.ds(0, nr - 1)]
    pltpu.make_async_copy(others_blk, others_blk, blk_recv).wait()
    for d in range(nr - 1, 0, -1):
        tell_rep(lax.rem(me_r + d, nr)).start()

    chunk = min(32, nb * PBLK_DEV, nr * pairs)
    flat = nb * SUBS
    tall = chunk * PR
    pair_row = mine[PBLK_DEV : PBLK_DEV + 1, :]
    grow = (div(iota((tall, chunk), 0), PR) == iota((tall, chunk), 1)).astype(BF16)
    in_row = mod(iota((tall, LANES), 0), PR) == mod(iota((tall, LANES), 1), PR)
    code_line = iota((1, CODES), 1).astype(F32)
    def code_of(spread_codes, book):
        pick = (div(iota((LANES, CODES), 0), PR) == book).astype(BF16)
        return dot(spread_codes, pick)

    def embed(select, heard):
        picked = dot(select.astype(BF16), heard)
        spread_codes = jnp.where(in_row, dot(grow, picked.astype(BF16)), 0.0).astype(BF16)
        quant = jnp.zeros((tall, feat), F32)
        for k in range(books):
            onehot = (code_of(spread_codes, k) == code_line).astype(BF16)
            quant = quant + dot(onehot, book_ref[pl.ds(k * CODES, CODES), :])
        inverse = lax.rsqrt(jnp.sum(quant * quant, axis=1, keepdims=True) + EPS)
        return spread_codes, quant * inverse, inverse

    heard_own = info[me_r].reshape(flat, LANES).astype(BF16)

    def own_chunk(c):
        row = iota((chunk, 1), 0) + c * chunk
        wide = iota((chunk, flat), 1)
        select = (div(wide, SUBS) == div(row, PBLK_DEV)) & (mod(wide, SUBS) == mod(row, PBLK_DEV))
        spread_codes, unit, inverse = embed(select, heard_own)
        own_unit[pl.ds(c * tall, tall), :] = unit
        own_inv[pl.ds(c * tall, tall), :] = jnp.broadcast_to(inverse, (tall, LANES))
        own_codes[pl.ds(c * tall, tall), :] = spread_codes

    loop(nb * PBLK_DEV // chunk, own_chunk)
    repeat = (iota((LANES, span), 0) == div(iota((LANES, span), 1), PR)).astype(BF16)
    directory = jnp.concatenate(
        [info[me_r, b][PBLK_DEV : PBLK_DEV + 1, :] for b in range(nb)], axis=0
    )
    blocks[...] = dot(directory.astype(BF16), repeat)

    pltpu.make_async_copy(others_rep, others_rep, rep_recv).wait()
    heard = info[...].reshape(nr * flat, LANES).astype(BF16)
    wide = iota((chunk, nr * flat), 1)
    from_dev = div(wide, SUBS)
    from_row = mod(wide, SUBS)

    def pair_chunk(c):
        row = iota((chunk, 1), 0) + c * chunk
        slot = mod(row, pairs)
        rep = div(row, pairs)
        block = jnp.sum(
            jnp.where(iota((chunk, LANES), 1) == slot, pair_row, 0.0), axis=1, keepdims=True
        ).astype(jnp.int32)
        select = (
            (mod(from_dev, nb) * PBLK_DEV + from_row == block)
            & (from_row < PBLK_DEV)
            & (div(from_dev, nb) == rep)
        )
        unused, unit, inverse = embed(select, heard)
        pair_unit[pl.ds(c * tall, tall), :] = unit.astype(BF16)

    loop(nr * pairs // chunk, pair_chunk)

    my_blocks = dot(jnp.broadcast_to(pair_row, (SUBS, LANES)).astype(BF16), repeat)[0:1, :]
    inner = mod(iota((1, span), 1), PR).astype(F32)
    column_ids = jnp.concatenate(
        [my_blocks * (PR * nr) + (inner + r * PR) for r in range(nr)], axis=1
    )
    eye = iota((rows, rows), 0) == iota((rows, rows), 1)
    goal = jnp.sum(
        jnp.where(eye, pos_ref[pl.ds(me_r, 1), :].astype(F32), 0.0), axis=1, keepdims=True
    )
    query = q_ref[...]
    unit_bf = pair_unit[...]
    scores = dot(query, unit_bf, ((1,), (1,)))
    hit = column_ids == goal
    peak = jnp.max(scores, axis=1, keepdims=True)
    lse = peak + jnp.log(jnp.sum(jnp.exp(scores - peak), axis=1, keepdims=True))
    target = jnp.sum(jnp.where(hit, scores, 0.0), axis=1, keepdims=True)
    weight = (jnp.exp(scores - lse) - hit.astype(F32)).astype(BF16)
    grad_cols = dot(weight, query, ((0,), (0,)))
    width = feat // PARTS
    for h in range(PARTS):
        piece = grad_cols[:, h * width : (h + 1) * width].astype(BF16)
        send2[h] = piece.reshape(nr, span, width)
    moves2 = []
    for h in range(PARTS):
        moves2.append([])
        for d in range(nr - 1, 0, -1):
            to = lax.rem(me_r + d, nr)
            move = pltpu.make_async_remote_copy(
                src_ref=send2.at[h, to], dst_ref=recv2.at[h, d],
                send_sem=s2.at[h, d], recv_sem=r2.at[h, d],
                device_id={"blk": me_b, "rep": to}, device_id_type=MESH,
            )
            move.start()
            moves2[h].append(move)
    loss_ref[...] = jnp.sum(jnp.where(eye, lse - target, 0.0), axis=0, keepdims=True)
    qgrad_ref[...] = dot(weight, unit_bf)

    peer = me_b + 1 - 2 * lax.rem(me_b, 2)
    half = nb // 2

    def share(h, slot, to, send_sem):
        return pltpu.make_async_remote_copy(
            src_ref=sums.at[h, slot], dst_ref=sums.at[h, slot], send_sem=send_sem,
            recv_sem=r3.at[h, slot], device_id={"blk": to, "rep": me_r}, device_id_type=MESH,
        )

    def add_block(h, b):
        line = blocks[pl.ds(b, 1), :].astype(jnp.int32)
        part = sums[h, b]

        def rows_chunk(c):
            row = iota((tall, span), 0) + c * tall
            select = (div(row, PR) == line) & (mod(row, PR) == mod(iota((tall, span), 1), PR))
            total[pl.ds(c * tall, tall), pl.ds(h * width, width)] += dot(select.astype(BF16), part)

        loop(nb * PBLK_DEV // chunk, rows_chunk)

    total[...] = jnp.zeros_like(total)
    for h in range(PARTS):
        for move in moves2[h]:
            move.wait()
        summed = send2[h, me_r].astype(F32)
        for d in range(1, nr):
            summed = summed + recv2[h, d].astype(F32)
        sums[h, me_b] = summed.astype(BF16)
        share(h, me_b, peer, s3.at[h, 0]).start()

        def send_far(k):
            share(h, me_b, lax.rem(me_b + 2 * (k + 1), nb), s3.at[h, k + 1]).start()

        loop(half - 1, send_far)
    for h in range(PARTS):
        add_block(h, me_b)
    for h in range(PARTS):

        def pass_on(k):
            slot = lax.rem(me_b + nb - 2 * (k + 1), nb)
            share(h, slot, peer, f3.at[h, k]).wait_recv()
            share(h, slot, peer, f3.at[h, k]).start()
            add_block(h, slot)

        loop(half - 1, pass_on)
    for h in range(PARTS):

        def take(k):
            slot = lax.rem(peer + nb - 2 * k, nb)
            share(h, slot, peer, s3.at[h, 0]).wait_recv()
            add_block(h, slot)

        loop(half, take)

    unit = own_unit[...]
    grad = total[...]
    grad = own_inv[:, 0:1] * (grad - unit * jnp.sum(unit * grad, axis=1, keepdims=True))
    total[...] = grad
    pgrad_ref[...] = total[pl.ds(me_b * own_rows, own_rows), :]

    group = send4.shape[0] * send4.shape[1]
    first = me_b * group
    wanted = code_of(own_codes[...], first // CODES)[:, 0:group]
    member = wanted == (iota((1, group), 1) + lax.rem(first, CODES)).astype(F32)
    part = dot(member.astype(BF16), grad.astype(BF16), ((0,), (0,)))
    send4[...] = part.astype(BF16).reshape(send4.shape)
    moves4 = []
    for d in range(nr - 1, 0, -1):
        to = lax.rem(me_r + d, nr)
        move = pltpu.make_async_remote_copy(
            src_ref=send4.at[to], dst_ref=recv4.at[d], send_sem=s4.at[d], recv_sem=r4.at[d],
            device_id={"blk": me_b, "rep": to}, device_id_type=MESH,
        )
        move.start()
        moves4.append(move)
    pltpu.make_async_copy(others_blk, others_blk, blk_send).wait()
    pltpu.make_async_copy(others_rep, others_rep, rep_send).wait()
    for h in range(PARTS):
        loop(half, lambda k: share(h, me_b, peer, s3.at[h, k]).wait_send())
        loop(half - 1, lambda k: share(h, me_b, peer, f3.at[h, k]).wait_send())
    for move in moves4:
        move.wait()
    summed = send4[me_r].astype(F32)
    for d in range(1, nr):
        summed = summed + recv4[d].astype(F32)
    cgrad_ref[...] = summed


def write_out(*refs):
    sems = refs[8]
    moves = [pltpu.make_async_copy(refs[k], refs[k + 4], sems.at[k]) for k in range(4)]
    for move in moves:
        move.start()
    for move in moves:
        move.wait()


def shards(query_embed, positive_ids, pair_blocks, code_ids, codebooks):
    nb = lax.axis_size("blk")
    nr = lax.axis_size("rep")
    rows, feat = query_embed.shape[2:]
    pairs = pair_blocks.shape[1]
    books = code_ids.shape[2]
    share_rows = codebooks.shape[0] // (nb * nr)
    span = pairs * PR
    passages = nb * PBLK_DEV * PR
    assert books * PR == LANES and codebooks.shape[0] == books * CODES and pairs <= LANES
    assert CODES % (share_rows * nr) == 0 and nb * PBLK_DEV <= 256 and CODES <= 256
    vmem = pl.BlockSpec(memory_space=pltpu.VMEM)
    hbm = pl.BlockSpec(memory_space=pltpu.HBM)
    dma = pltpu.SemaphoreType.DMA
    limit = 67_000_000 if nb * span * feat > 8_000_000 else 32_000_000
    shapes = (
        jax.ShapeDtypeStruct((1, rows), F32),
        jax.ShapeDtypeStruct((rows, feat), F32),
        jax.ShapeDtypeStruct((PBLK_DEV * PR, feat), F32),
        jax.ShapeDtypeStruct((share_rows, feat), F32),
    )
    outs = pl.pallas_call(
        functools.partial(kernel, nb, nr, pairs),
        out_shape=shapes,
        in_specs=[vmem] * 5,
        out_specs=(vmem,) * 4,
        scratch_shapes=[
            pltpu.VMEM((nr, nb, SUBS, LANES), F32),
            pltpu.VMEM((nr * span, feat), BF16),
            pltpu.VMEM((passages, feat), F32),
            pltpu.VMEM((passages, LANES), F32),
            pltpu.VMEM((passages, LANES), BF16),
            pltpu.VMEM((PARTS, nr, span, feat // PARTS), BF16),
            pltpu.VMEM((PARTS, nr, span, feat // PARTS), BF16),
            pltpu.VMEM((PARTS, nb, span, feat // PARTS), BF16),
            pltpu.VMEM((nb, span), F32),
            pltpu.VMEM((passages, feat), F32),
            pltpu.VMEM((nr, share_rows, feat), BF16),
            pltpu.VMEM((nr, share_rows, feat), BF16),
            dma, dma, dma, dma, dma((PARTS, nr)), dma((PARTS, nr)),
            dma((PARTS, nb // 2)), dma((PARTS, nb // 2)), dma((PARTS, nb)), dma((nr,)), dma((nr,)),
        ],
        compiler_params=pltpu.CompilerParams(
            has_side_effects=True, collective_id=0, vmem_limit_bytes=limit
        ),
    )(query_embed[0, 0], positive_ids[0], pair_blocks, code_ids[0, 0], codebooks)
    loss, query_grad, passage_grad, codebook_grad = pl.pallas_call(
        write_out,
        out_shape=shapes,
        in_specs=[vmem] * 4,
        out_specs=(hbm,) * 4,
        scratch_shapes=[dma((4,))],
        compiler_params=pltpu.CompilerParams(vmem_limit_bytes=8_000_000),
    )(*outs)
    return (loss[None], query_grad[None, None], passage_grad[None, None], codebook_grad)


def solution(mesh):
    placed = (
        P("blk", "rep", None, None),
        P("blk", None, None),
        P("blk", None),
        P("blk", "rep", None, None),
        P(),
    )
    return jax.shard_map(
        shards,
        mesh=mesh,
        in_specs=placed,
        out_specs=(
            P("blk", "rep", None),
            P("blk", "rep", None, None),
            P("blk", "rep", None, None),
            P(("blk", "rep"), None),
        ),
        check_vma=False,
    )
```
